32 devices in a mesh: ep: 16 (over z, x, core), dp: 2 (over y).
Axes of the slice: x: 2, y: 2, z: 4, core: 2. Of those that a mesh axis runs over, the one named last changes fastest.
Arguments:
- tokens: bfloat16 [256, 3584], P('ep'), may hold values from -6 to 6
- expert_ids: int32 [256, 8], P('ep'), may hold values from 0 to 15, all different within a row; in each aligned block of 16 rows (0 to 15, 16 to 31, ...) at most 16 rows name the same one
- route_logits: float32 [256, 8], P('ep'), may hold values from -8 to 8
- expert_gate: bfloat16 [16, 3584, 1024], P('ep', None, 'dp'), may hold values from -0.09375 to 0.09375
- expert_up: bfloat16 [16, 3584, 1024], P('ep', None, 'dp'), may hold values from -0.09375 to 0.09375
- expert_down: bfloat16 [16, 1024, 3584], P('ep', 'dp'), may hold values from -0.1875 to 0.1875
Outputs:
- mixed: bfloat16 [256, 3584], P(('ep', 'dp'))
The draws below stay inside these ranges and needn't reach their ends.
Inputs may be any that keep to these rules, and one draw needn't show every extreme that they name: `expert_ids`: each row names 8 different experts of 0 to 15 and every expert is named by some row. Within the rows of one index of ep (aligned blocks of 16 rows) no expert is named more than 16 times, and some block names one expert exactly 16 times. Loads are heavy-tailed: a few experts take several times the mean.
All inputs are finite; a program needn't handle non-finite values.
Results may differ from the reference program's by a relative error of at most 0.015.
Values may be sent and summed in bfloat16 or wider, within the bound.
A program may use at most 64 MiB of HBM per device.

```python
import math
import jax
import jax.numpy as jnp
import numpy as np
from jax import lax

D = 3584
FF = 1024
TOP = 8
TOK_EP = 16
EXPERTS = 16
TOKENS = 256
CAP = 16


def block_levels(own_key, shape, cuts, smallest, largest):
    gain = 1.0
    for position, parts in cuts:
        steps = jax.random.uniform(jax.random.fold_in(jax.random.fold_in(own_key, 6), position), (parts,), jnp.float32, smallest / len(cuts), largest / len(cuts))
        gain = gain * jnp.repeat(jnp.exp(steps), shape[position] // parts).reshape((-1,) + (1,) * (len(shape) - 1 - position))
    return gain


def deal_out(key, own, number, rows, amount, top, reach, lean):
    sequence = jax.random.permutation(key, amount)
    heavy_load, usual = load_shares(amount, rows * top, reach, lean, True), load_shares(amount, rows * top, reach, lean, False)
    places = jnp.arange(amount)

    def named(tallies, rotation):
        used = int((tallies > 0).sum())
        fixed = max(1, used // 4)
        shifted = fixed + (places - fixed + rotation * (used - fixed)) % max(1, amount - fixed)
        return jnp.zeros((amount,), jnp.int32).at[sequence[jnp.where(places < fixed, places, shifted)]].set(jnp.asarray(tallies, jnp.int32))

    tallies = jnp.where(number % 4 == 0, named(heavy_load, number // 4), named(usual, number - number // 4 - 1))
    mixed = jax.random.permutation(jax.random.fold_in(own, 3), amount)
    donor, taker = mixed[0:amount // 2 * 2:2], mixed[1:amount // 2 * 2:2]
    margin = jnp.minimum(tallies[donor] - 1, reach - tallies[taker]) // 2
    margin = jnp.where((donor == sequence[0]) | (taker == sequence[0]) | (tallies[taker] == 0), 0, jnp.maximum(margin, 0))
    shifted = jax.random.randint(jax.random.fold_in(own, 4), (amount // 2,), 0, 1 << 20) % (margin + 1)
    tallies = tallies.at[donor].add(-shifted).at[taker].add(shifted)
    members = jnp.searchsorted(jnp.cumsum(tallies), jnp.arange(rows * top), side="right").astype(jnp.int32)
    listing = members.reshape(top, rows).T
    listing = listing[jax.random.permutation(jax.random.fold_in(own, 1), rows)]
    rotation = jax.random.randint(jax.random.fold_in(own, 2), (rows, 1), 0, top)
    return jnp.take_along_axis(listing, (jnp.arange(top)[None, :] + rotation) % top, axis=1)


def load_shares(count, total, bound, slope, full):
    loads = [(1 << 20) // math.isqrt(standing ** slope) + 1 for standing in range(1, count + 1)]
    largest = bound if full else min(bound, max(-(-total // count), total * loads[0] // sum(loads)))
    least = 1 if total - largest >= count - 1 else 0
    given, spare = [largest] + [least] * (count - 1), total - largest - least * (count - 1)
    while spare > 0:
        free = [i for i in range(1, count) if given[i] < largest] or [i for i in range(1, count) if given[i] < bound]
        pool, remaining = sum([loads[i] for i in free]), spare
        for i in free:
            extra = min(bound - given[i], max(1, remaining * loads[i] // pool), spare)
            given[i] = given[i] + extra
            spare = spare - extra
    return np.array(given)


def scatter_about(rng, extent, scale, most, cuts=(), held_as=jnp.bfloat16):
    result = jax.random.normal(rng, extent, jnp.float32) * scale
    if len(cuts) > 0:
        result = block_levels(rng, extent, cuts, -0.22, 0.18) * result
    return jnp.clip(result, min=-most, max=most).astype(held_as)


def setup_inputs(seed: int = 0) -> dict:
    key_of = jax.random.split(jax.random.key(seed), 7)
    tokens = scatter_about(key_of[0], (TOKENS, D), 1.0, 6.0, ((0, 16),))
    expert_ids_keys = jax.random.split(jax.random.fold_in(key_of[1], 1), TOKENS // TOK_EP)
    expert_ids_turns = jax.random.permutation(jax.random.fold_in(key_of[1], 3), TOKENS // TOK_EP)
    expert_ids = jax.vmap(lambda own, number: deal_out(jax.random.fold_in(key_of[1], 2), own, number, TOK_EP, EXPERTS, TOP, CAP, 3))(expert_ids_keys, expert_ids_turns).reshape((TOKENS, TOP))
    route_logits = scatter_about(key_of[2], (TOKENS, TOP), 2.0, 8.0, ((0, 16),), jnp.float32)
    expert_gate = scatter_about(key_of[3], (EXPERTS, D, FF), D ** -0.5, 0.09375, ((0, 16), (2, 2)))
    expert_up = scatter_about(key_of[4], (EXPERTS, D, FF), D ** -0.5, 0.09375, ((0, 16), (2, 2)))
    expert_down = scatter_about(key_of[5], (EXPERTS, FF, D), FF ** -0.5, 0.1875, ((0, 16), (1, 2)))
    return dict(tokens=tokens, expert_ids=expert_ids, route_logits=route_logits, expert_gate=expert_gate, expert_up=expert_up, expert_down=expert_down)


route_scale = 2.5


def expert_rows(rows, w_gate, w_up, w_down):
    gate = jnp.dot(rows, w_gate, preferred_element_type=jnp.float32)
    upper = jnp.dot(rows, w_up, preferred_element_type=jnp.float32)
    hidden = (jax.nn.silu(gate) * upper).astype(jnp.bfloat16)
    return jnp.dot(hidden, w_down, preferred_element_type=jnp.float32).astype(jnp.bfloat16)


def reference(tokens, expert_ids, route_logits, expert_gate, expert_up, expert_down):
    token_count, width = tokens.shape
    top = expert_ids.shape[1]
    experts = expert_gate.shape[0]
    flat_ids = expert_ids.reshape(-1).astype(jnp.int32)
    slots = flat_ids.shape[0]
    block_rows = 64
    counts = jnp.zeros((experts,), jnp.int32).at[flat_ids].add(1).astype(jnp.int32)
    padded = (((counts + block_rows - 1) // block_rows) * block_rows).astype(jnp.int32)
    pad_start = (jnp.cumsum(padded) - padded).astype(jnp.int32)
    seg_start = (jnp.cumsum(counts) - counts).astype(jnp.int32)
    sorted_slots = jnp.argsort(flat_ids, stable=True).astype(jnp.int32)
    sorted_ids = flat_ids[sorted_slots]
    within = (jnp.arange(slots, dtype=jnp.int32) - seg_start[sorted_ids]).astype(jnp.int32)
    target = (pad_start[sorted_ids] + within).astype(jnp.int32)
    nblocks = (slots + experts * (block_rows - 1)) // block_rows + 1
    row_token = jnp.full((nblocks * block_rows,), token_count, jnp.int32).at[target].set((sorted_slots // top).astype(jnp.int32))
    pad_end = pad_start + padded
    block_start = jnp.arange(nblocks, dtype=jnp.int32) * block_rows
    block_expert = jnp.sum((pad_end[None, :] <= block_start[:, None]).astype(jnp.int32), axis=1)
    block_expert = jnp.minimum(block_expert, experts - 1).astype(jnp.int32)
    extended = jnp.concatenate([tokens, jnp.zeros((1, width), tokens.dtype)], axis=0)

    def one_block(inputs):
        block_index, expert = inputs
        picks = lax.dynamic_slice_in_dim(row_token, (block_index * block_rows).astype(jnp.int32), block_rows, 0)
        return expert_rows(extended[picks], expert_gate[expert], expert_up[expert], expert_down[expert])

    outputs = lax.map(one_block, (jnp.arange(nblocks, dtype=jnp.int32), block_expert))
    outputs = outputs.reshape(nblocks * block_rows, width)
    slot_target = jnp.zeros((slots,), jnp.int32).at[sorted_slots].set(target)
    slot_values = outputs[slot_target].reshape(token_count, top, width)
    scores = jax.nn.sigmoid(route_logits)
    weights = route_scale * scores / jnp.sum(scores, axis=1, keepdims=True)
    routed = jnp.sum(weights[:, :, None] * slot_values.astype(jnp.float32), axis=1)
    return routed.astype(jnp.bfloat16)
```

```python
import functools

import jax
import jax.numpy as jnp
from jax import lax
from jax.experimental import pallas as pl
from jax.experimental.pallas import tpu as pltpu
from jax.sharding import PartitionSpec as P

route_scale = 2.5


def by_slots(tokens, expert_ids, route_logits, expert_gate, expert_up, expert_down):
    tok_rows, width = tokens.shape
    top = expert_ids.shape[1]
    n_ep = lax.axis_size("ep")
    n_dp = lax.axis_size("dp")
    experts = n_ep
    capacity = min(tok_rows, 4 * max(1, tok_rows * top // experts))
    flat_ids = expert_ids.reshape(-1).astype(jnp.int32)
    onehot = (flat_ids[:, None] == jnp.arange(experts, dtype=jnp.int32)[None, :]).astype(jnp.int32)
    earlier = jnp.cumsum(onehot, axis=0).astype(jnp.int32) - onehot
    within = jnp.sum(earlier * onehot, axis=1).astype(jnp.int32)
    slot_index = flat_ids * capacity + within
    token_of_slot = jnp.arange(tok_rows * top, dtype=jnp.int32) // top
    source_row = (
        jnp.full((experts * capacity,), tok_rows, jnp.int32).at[slot_index].set(token_of_slot)
    )
    extended = jnp.concatenate([tokens, jnp.zeros((1, width), tokens.dtype)], axis=0)
    outgoing = extended[source_row].reshape(n_ep, capacity, width)
    arrived = lax.all_to_all(outgoing, "ep", split_axis=0, concat_axis=0, tiled=True)
    received = arrived.reshape(n_ep * capacity, width)
    gate = jnp.dot(received, expert_gate[0], preferred_element_type=jnp.float32)
    upper = jnp.dot(received, expert_up[0], preferred_element_type=jnp.float32)
    hidden = (jax.nn.silu(gate) * upper).astype(jnp.bfloat16)
    partial_value = jnp.dot(hidden, expert_down[0], preferred_element_type=jnp.float32)
    partial_value = partial_value.reshape(n_ep, capacity, width)
    scores = jax.nn.sigmoid(route_logits)
    weights = route_scale * scores / jnp.sum(scores, axis=1, keepdims=True)
    member = lax.axis_index("dp")
    quarter = capacity // n_dp
    reduced = (
        lax.psum_scatter(partial_value.astype(jnp.bfloat16), "dp", scatter_dimension=1, tiled=True)
        .astype(jnp.float32)
        .astype(jnp.bfloat16)
    )
    back = lax.all_to_all(reduced, "ep", split_axis=0, concat_axis=0, tiled=True)
    offset = within - member * quarter
    held = ((offset >= 0) & (offset < quarter)).astype(jnp.float32)
    picked = flat_ids * quarter + jnp.clip(offset, 0, quarter - 1)
    values = back.reshape(experts * quarter, width)[picked].reshape(tok_rows, top, width)
    masked = weights * held.reshape(tok_rows, top)
    contrib = jnp.sum(masked[:, :, None] * values.astype(jnp.float32), axis=1)
    routed = lax.psum_scatter(
        contrib.astype(jnp.bfloat16), "dp", scatter_dimension=0, tiled=True
    ).astype(jnp.float32)
    return routed.astype(jnp.bfloat16)


MESH = pl.DeviceIdType.MESH
LANES = 128
RIGHT, LEFT, ACROSS, SIDE, CORE = range(5)


def exchange_kernel(
    planes, tokens_ref, ids_ref, logits_ref, gate_hbm, up_hbm, down_hbm, out_ref,
    tok, w_gate, w_up, w_down, hid, wcol, theirs, part, from_core, from_first, line_out, line_in,
    last_out, last_in,
    weight_sem, tok_send, tok_recv, core_send, core_recv, first_send, first_recv,
    line_send, line_recv, last_send, last_recv,
):
    rows, width = tokens_ref.shape
    top = ids_ref.shape[1]
    hidden = gate_hbm.shape[2]
    wide = tok.shape[1]
    half = wide // 2
    sub = rows // 2
    me, y = lax.axis_index("ep"), lax.axis_index("dp")
    c, x, z = me % 2, (me // 2) % 2, me // 4

    def ep_of(zz, xx, cc):
        return (zz * 2 + xx) * 2 + cc

    def device(kind):
        if kind == RIGHT:
            return (ep_of(z + 1, x, c), y)
        if kind == LEFT:
            return (ep_of(z - 1, x, c), y)
        if kind == ACROSS:
            return (ep_of(z, 1 - x, c), y)
        if kind == SIDE:
            return (me, 1 - y)
        return (ep_of(z, x, 1 - c), y)

    loads = [
        pltpu.make_async_copy(src.at[0], dst, weight_sem.at[i])
        for i, (src, dst) in enumerate(((gate_hbm, w_gate), (up_hbm, w_up), (down_hbm, w_down)))
    ]
    for load in loads:
        load.start()

    barrier = pltpu.get_barrier_semaphore()

    def greet(kind):
        pl.semaphore_signal(barrier, inc=1, device_id=device(kind), device_id_type=MESH)

    for kind in (ACROSS, SIDE, CORE):
        greet(kind)
    pl.when(z > 0)(lambda: greet(LEFT))
    pl.when(z < planes - 1)(lambda: greet(RIGHT))

    scores = jax.nn.sigmoid(logits_ref[...])
    weights = route_scale * scores / jnp.sum(scores, axis=1, keepdims=True)
    lane = lax.broadcasted_iota(jnp.int32, (rows, LANES), 1)
    dense = jnp.zeros((rows, LANES), jnp.float32)
    for k in range(top):
        dense = dense + jnp.where(lane == ids_ref[:, k : k + 1], weights[:, k : k + 1], 0.0)
    coarse = dense.astype(jnp.bfloat16)
    fine = (dense - coarse.astype(jnp.float32)).astype(jnp.bfloat16)
    own_rows = pl.ds(pl.multiple_of(me * rows, rows), rows)
    tok[own_rows, :width] = tokens_ref[...]
    tok[own_rows, width : width + LANES] = coarse
    tok[own_rows, width + LANES :] = fine

    middle = jnp.where(z > 0, 1, 0) + jnp.where(z < planes - 1, 1, 0)
    pl.semaphore_wait(barrier, 3 + middle)

    def unit(block, h):
        return tok.at[
            pl.ds(pl.multiple_of(block * rows, rows), rows),
            pl.ds(pl.multiple_of(h * half, LANES), half),
        ]

    def token_copy(kind, block, h):
        return pltpu.make_async_remote_copy(
            src_ref=unit(block, h),
            dst_ref=unit(block, h),
            send_sem=tok_send.at[kind, block, h],
            recv_sem=tok_recv.at[block, h],
            device_id=device(kind),
            device_id_type=MESH,
        )

    def on_line(do, arrived, d, k):
        h = y if k == 0 else 1 - y

        def pass_on(block, right, left):
            if arrived:
                token_copy(CORE, block, h).wait_recv()
            if right:
                pl.when(z < planes - 1)(lambda: do(token_copy(RIGHT, block, h)))
            if left:
                pl.when(z > 0)(lambda: do(token_copy(LEFT, block, h)))
            if k == 0:
                do(token_copy(ACROSS, block, h))
            do(token_copy(CORE, block, h))

        if d == 0:
            pass_on(me, True, True)
        else:
            pl.when(z - d >= 0)(lambda: pass_on(ep_of(z - d, x, c), True, False))
            pl.when(z + d < planes)(lambda: pass_on(ep_of(z + d, x, c), False, True))

    def at_distance(d, act):
        if d == 0:
            act(z)
        else:
            pl.when(z - d >= 0)(lambda: act(z - d))
            pl.when(z + d < planes)(lambda: act(z + d))

    def token_moves(do, arrived):
        for step in range(planes + 2):
            if step < planes:
                for k in range(2):
                    on_line(do, arrived and step > 0, step, k)
            if 0 <= step - 1 < planes:

                def crossed(zz):
                    block = ep_of(zz, 1 - x, c)
                    if arrived:
                        token_copy(CORE, block, y).wait_recv()
                    do(token_copy(SIDE, block, y))
                    do(token_copy(CORE, block, y))

                at_distance(step - 1, crossed)
            if 0 <= step - 2 < planes:

                def sided(zz):
                    block = ep_of(zz, 1 - x, c)
                    if arrived:
                        token_copy(CORE, block, 1 - y).wait_recv()
                    do(token_copy(CORE, block, 1 - y))

                at_distance(step - 2, sided)

    token_moves(lambda copy: copy.start(), True)
    for zz in range(planes):
        for xx in range(2):
            for h in range(2):
                token_copy(CORE, ep_of(zz, xx, 1 - c), h).wait_recv()

    loads[0].wait()
    loads[1].wait()
    step_f = 256

    def project(i, carry):
        cols = pl.ds(pl.multiple_of(i * step_f, step_f), step_f)
        gate = jnp.dot(tok[:, :width], w_gate[:, cols], preferred_element_type=jnp.float32)
        upper = jnp.dot(tok[:, :width], w_up[:, cols], preferred_element_type=jnp.float32)
        value = (gate / (1.0 + jnp.exp(-gate)) * upper).astype(jnp.bfloat16)
        value = value.reshape(planes * 2, 2, rows, step_f)
        for cc in range(2):
            hid[cc, :, cols] = value[:, cc].reshape(planes * 2 * rows, step_f)
        return carry

    lax.fori_loop(0, hidden // step_f, project, 0)

    table = tok[:, width : width + LANES].astype(jnp.float32) + tok[:, width + LANES :].astype(
        jnp.float32
    )
    every = lax.broadcasted_iota(jnp.int32, table.shape, 1)
    chosen = jnp.sum(jnp.where(every == me, table, 0.0), axis=1, keepdims=True)
    chosen = jnp.broadcast_to(chosen, table.shape).reshape(planes * 2, 2, rows, LANES)
    for cc in range(2):
        wcol[cc] = chosen[:, cc].reshape(planes * 2 * rows, LANES)

    loads[2].wait()
    step_n = 512

    def expand(cc, dst):
        def one(i, carry):
            cols = pl.ds(pl.multiple_of(i * step_n, step_n), step_n)
            value = jnp.dot(hid[cc], w_down[:, cols], preferred_element_type=jnp.float32)
            value = value * wcol[cc][:, :1]
            for zz in range(planes):
                for xx in range(2):
                    for yy in range(2):
                        first = jnp.where(cc == 0, yy, xx)
                        second = jnp.where(cc == 0, xx, yy)
                        at = ((zz * 2 + xx) * 2 + yy) * sub
                        dst[zz, first, second, :, cols] = value[at : at + sub].astype(jnp.bfloat16)
            return carry

        lax.fori_loop(0, width // step_n, one, 0)

    def core_copy(t):
        return pltpu.make_async_remote_copy(
            src_ref=theirs.at[t], dst_ref=from_core.at[t],
            send_sem=core_send.at[t], recv_sem=core_recv.at[t],
            device_id=device(CORE), device_id_type=MESH,
        )

    expand(1 - c, theirs)
    for d in range(planes - 1, -1, -1):
        at_distance(d, lambda t: core_copy(t).start())
    expand(c, part)

    a = jnp.where(c == 0, y, x)
    b = jnp.where(c == 0, x, y)
    swap_y = (me, 1 - y)
    swap_x = (ep_of(z, 1 - x, c), y)
    first_device = tuple(jnp.where(c == 0, p, q) for p, q in zip(swap_y, swap_x))
    last_device = tuple(jnp.where(c == 0, q, p) for p, q in zip(swap_y, swap_x))

    def first_copy(t):
        return pltpu.make_async_remote_copy(
            src_ref=part.at[t, 1 - a], dst_ref=from_first.at[t],
            send_sem=first_send.at[t], recv_sem=first_recv.at[t],
            device_id=first_device, device_id_type=MESH,
        )

    def add_core(t):
        core_copy(t).wait_recv()
        part[t] = (part[t].astype(jnp.float32) + from_core[t].astype(jnp.float32)).astype(
            jnp.bfloat16
        )
        first_copy(t).start()

    for d in range(planes - 1, -1, -1):
        at_distance(d, add_core)

    def line_copy(side, t):
        return pltpu.make_async_remote_copy(
            src_ref=line_out.at[t], dst_ref=line_in.at[side, t],
            send_sem=line_send.at[t], recv_sem=line_recv.at[side, t],
            device_id=device(RIGHT if side == 0 else LEFT), device_id_type=MESH,
        )

    def kept(t):
        first_copy(t).wait_recv()
        return part[t, a].astype(jnp.float32) + from_first[t].astype(jnp.float32)

    def relay(side, t):
        line_out[t] = kept(t).astype(jnp.bfloat16)
        inner = z > 0 if side == 0 else z < planes - 1

        @pl.when(inner)
        def _():
            line_copy(side, t).wait_recv()
            line_out[t] = (
                line_out[t].astype(jnp.float32) + line_in[side, t].astype(jnp.float32)
            ).astype(jnp.bfloat16)

        line_copy(side, t).start()

    for d in range(planes - 1, 0, -1):
        pl.when(z + d < planes)(lambda: relay(0, z + d))
        pl.when(z - d >= 0)(lambda: relay(1, z - d))

    last_out[...] = kept(z)

    def gathered(side):
        line_copy(side, z).wait_recv()
        last_out[...] = last_out[...] + line_in[side, z].astype(jnp.float32)

    pl.when(z > 0)(lambda: gathered(0))
    pl.when(z < planes - 1)(lambda: gathered(1))
    line_out[z] = last_out[...].astype(jnp.bfloat16)
    final = pltpu.make_async_remote_copy(
        src_ref=line_out.at[z, 1 - b], dst_ref=last_in,
        send_sem=last_send, recv_sem=last_recv,
        device_id=last_device, device_id_type=MESH,
    )
    final.start()
    final.wait_recv()
    out_ref[...] = (last_out[b] + last_in[...].astype(jnp.float32)).astype(out_ref.dtype)

    final.wait_send()
    token_moves(lambda copy: copy.wait_send(), False)
    for t in range(planes):
        core_copy(t).wait_send()
        first_copy(t).wait_send()
    for d in range(1, planes):
        pl.when(z + d < planes)(lambda: line_copy(0, z + d).wait_send())
        pl.when(z - d >= 0)(lambda: line_copy(1, z - d).wait_send())


def by_gather(tokens, expert_ids, route_logits, expert_gate, expert_up, expert_down):
    rows, width = tokens.shape
    hidden = expert_gate.shape[2]
    n_ep, n_dp = lax.axis_size("ep"), lax.axis_size("dp")
    planes = n_ep // 4
    wide = width + 2 * LANES
    sub = rows // n_dp
    vmem = pl.BlockSpec(memory_space=pltpu.VMEM)
    anywhere = pl.BlockSpec(memory_space=pl.ANY)
    bf16, f32, dma = jnp.bfloat16, jnp.float32, pltpu.SemaphoreType.DMA
    return pl.pallas_call(
        functools.partial(exchange_kernel, planes),
        out_shape=jax.ShapeDtypeStruct((sub, width), bf16),
        in_specs=[vmem, vmem, vmem, anywhere, anywhere, anywhere],
        out_specs=vmem,
        scratch_shapes=[
            pltpu.VMEM((n_ep * rows, wide), bf16),
            pltpu.VMEM((width, hidden), bf16),
            pltpu.VMEM((width, hidden), bf16),
            pltpu.VMEM((hidden, width), bf16),
            pltpu.VMEM((2, n_ep * rows // 2, hidden), bf16),
            pltpu.VMEM((2, n_ep * rows // 2, LANES), f32),
            pltpu.VMEM((planes, 2, 2, sub, width), bf16),
            pltpu.VMEM((planes, 2, 2, sub, width), bf16),
            pltpu.VMEM((planes, 2, 2, sub, width), bf16),
            pltpu.VMEM((planes, 2, sub, width), bf16),
            pltpu.VMEM((planes, 2, sub, width), bf16),
            pltpu.VMEM((2, planes, 2, sub, width), bf16),
            pltpu.VMEM((2, sub, width), f32),
            pltpu.VMEM((sub, width), bf16),
            dma((3,)),
            dma((5, n_ep, 2)),
            dma((n_ep, 2)),
            dma((planes,)),
            dma((planes,)),
            dma((planes,)),
            dma((planes,)),
            dma((planes,)),
            dma((2, planes)),
            dma,
            dma,
        ],
        compiler_params=pltpu.CompilerParams(
            collective_id=0, has_side_effects=True, vmem_limit_bytes=56 * 1024 * 1024
        ),
    )(tokens, expert_ids, route_logits, expert_gate, expert_up, expert_down)


def on_device(tokens, expert_ids, route_logits, expert_gate, expert_up, expert_down):
    rows, width = tokens.shape
    n_ep, n_dp = lax.axis_size("ep"), lax.axis_size("dp")
    crowded = 4 * max(1, rows * expert_ids.shape[1] // n_ep) >= rows
    fits = n_dp == 2 and n_ep % 4 == 0 and n_ep <= LANES and rows == 16 and width % 512 == 0
    fits = fits and expert_gate.shape[0] == 1 and expert_gate.shape[2] % 256 == 0
    run = by_gather if crowded and fits else by_slots
    return run(tokens, expert_ids, route_logits, expert_gate, expert_up, expert_down)


def solution(mesh):
    placed = (
        P("ep", None),
        P("ep", None),
        P("ep", None),
        P("ep", None, "dp"),
        P("ep", None, "dp"),
        P("ep", "dp", None),
    )
    return jax.shard_map(
        on_device, mesh=mesh, in_specs=placed, out_specs=P(("ep", "dp"), None), check_vma=False
    )
```
